32 devices in a mesh: dp: 8 (over z, y), mp: 4 (over x, core).
Axes of the slice: x: 2, y: 2, z: 4, core: 2. Of those that a mesh axis runs over, the one named last changes fastest.
Arguments:
- slow_weights: float32 [1, 3584, 1024], P(None, None, 'mp'), may hold values from -6 to 6
- fast_weights: bfloat16 [8, 1, 3584, 1024], P('dp', None, None, 'mp'), may hold values from -64 to 64
- momentum: float32 [1, 3584, 1024], P(None, None, 'mp'), may hold values from -1.2 to 1.2
Outputs:
- slow_next: float32 [1, 3584, 1024], P(None, None, 'mp')
- momentum_next: float32 [1, 3584, 1024], P(None, None, 'mp')
- fast_next: bfloat16 [8, 1, 3584, 1024], P('dp', None, None, 'mp')
The draws below stay inside these ranges and needn't reach their ends.
All inputs are finite; a program needn't handle non-finite values.
Results may differ from the reference program's by a relative error of at most 0.001.
Values sent between devices are 32-bit elements; how exact they have to be, the bound alone decides.
No kernel may reach another device: no remote copies, remote signals or barrier semaphores. Data moves between devices by JAX's collectives and lax.ppermute only.
A program may use at most 64 MiB of HBM per device.

```python
import math
import jax
import jax.numpy as jnp
from jax import lax

D = 3584
LAYERS = 1
KV2 = 1024
REPLICAS = 8


def slow_base(key):
    values = jax.random.normal(jax.random.fold_in(key, 11), (LAYERS, D, KV2), jnp.float32)
    return jnp.clip(values, -6.0, 6.0)


def draw_slow_weights(key, part):
    return slow_base(key)


def draw_fast_weights(key, part):
    slow_values = slow_base(key)
    row_place = jnp.arange(D, dtype=jnp.float32) / D
    col_place = jnp.arange(KV2, dtype=jnp.float32) / KV2
    row_spread = 10.0 ** jax.random.uniform(jax.random.fold_in(key, 12), (D,), jnp.float32)
    col_spread = 10.0 ** jax.random.uniform(jax.random.fold_in(key, 13), (KV2,), jnp.float32)
    common = jax.random.normal(jax.random.fold_in(key, 14), (LAYERS, D, KV2), jnp.float32)
    single = jax.random.normal(jax.random.fold_in(key, 15), (REPLICAS, LAYERS, D, KV2), jnp.float32)
    row_scale = (1.0 + 2.0 * row_place) * row_spread
    col_scale = (1.0 + 2.0 * col_place) * col_spread
    drift = 0.02 * (common[None] + 1.5 * single)
    drift = drift * row_scale[:, None] * col_scale[None, :]
    fast_values = jnp.clip(slow_values[None] - drift, -64.0, 64.0)
    return fast_values.astype(jnp.bfloat16)


def shard_levels(rng, extent, cuts, least, high):
    factor_of = 1.0
    for axis_at, shards_of in cuts:
        heights = jax.random.uniform(jax.random.fold_in(jax.random.fold_in(rng, 6), axis_at), (shards_of,), jnp.float32, least / len(cuts), high / len(cuts))
        factor_of = factor_of * jnp.repeat(jnp.exp(heights), extent[axis_at] // shards_of).reshape((-1,) + (1,) * (len(extent) - 1 - axis_at))
    return factor_of


def gaussian(own_key, dims, deviation, reach, pieces=(), kind=jnp.bfloat16):
    result = jax.random.normal(own_key, dims, jnp.float32) * deviation
    if len(pieces) > 0:
        result = shard_levels(own_key, dims, pieces, -0.22, 0.18) * result
    return jnp.clip(result, min=-reach, max=reach).astype(kind)


def setup_inputs(seed: int = 0) -> dict:
    splits = jax.random.split(jax.random.key(seed), 4)
    return {
        "slow_weights": draw_slow_weights(jax.random.fold_in(splits[3], 71), 0),
        "fast_weights": draw_fast_weights(jax.random.fold_in(splits[3], 71), 0),
        "momentum": gaussian(splits[2], (LAYERS, D, KV2), 0.2, 1.2, ((2, 4),), jnp.float32),
    }


MOMENTUM_RATE = 0.9
OUTER_RATE = 0.7
CLIP_LEVEL = 0.2
EPSILON = 1e-06

def reference(slow_weights, fast_weights, momentum):

    def accumulate(summed, fast_one):
        return (summed + (slow_weights - fast_one.astype(jnp.float32)), None)
    summed, unused = lax.scan(accumulate, jnp.zeros_like(slow_weights), fast_weights)
    pseudo = summed / REPLICAS
    norm_value = jnp.sqrt(jnp.sum(pseudo * pseudo))
    max_norm = CLIP_LEVEL * math.sqrt(LAYERS * D * KV2)
    factor = jnp.minimum(1.0, max_norm / (norm_value + EPSILON))
    gradient = factor * pseudo
    momentum_next = MOMENTUM_RATE * momentum + gradient
    slow_next = slow_weights - OUTER_RATE * (gradient + MOMENTUM_RATE * momentum_next)
    fast_next = jnp.broadcast_to(slow_next.astype(jnp.bfloat16)[None], fast_weights.shape)
    return (slow_next, momentum_next, fast_next)
```

```python
import functools
import math

import jax
import jax.numpy as jnp
from jax import lax
from jax.experimental import pallas as pl
from jax.experimental.pallas import tpu as pltpu
from jax.sharding import PartitionSpec as P

MOMENTUM_RATE = 0.9
OUTER_RATE = 0.7
CLIP_LEVEL = 0.2
EPSILON = 1e-06
STREAMS = 2
VMEM = pl.BlockSpec(memory_space=pltpu.VMEM)
SMEM = pl.BlockSpec(memory_space=pltpu.SMEM)
HBM = pl.BlockSpec(memory_space=pltpu.HBM)


def piece_index(place_ref, n, back, s):
    return lax.rem(place_ref[0] + place_ref[1] * back + 2 * n, n) * STREAMS + s


def estimate(elements, bytes_each, flops_each):
    return pl.CostEstimate(
        flops=flops_each * elements, bytes_accessed=bytes_each * elements, transcendentals=0
    )


def grant(elements, bytes_each):
    return pltpu.CompilerParams(vmem_limit_bytes=elements * bytes_each + (1 << 20))


def first_kernel(n, place_ref, slow_ref, fast_ref, *refs):
    outs, (slow_buf, fast_buf, sems) = refs[:STREAMS], refs[STREAMS:]
    copies = []
    for s in range(STREAMS):
        index = piece_index(place_ref, n, 1, s)
        a = pltpu.make_async_copy(slow_ref.at[index], slow_buf.at[s], sems.at[0, s])
        b = pltpu.make_async_copy(fast_ref.at[index], fast_buf.at[s], sems.at[1, s])
        a.start()
        b.start()
        copies.append((a, b))
    for s, (a, b) in enumerate(copies):
        a.wait()
        b.wait()
        outs[s][...] = slow_buf[s] - fast_buf[s].astype(jnp.float32)


def first_pieces(place, slow, fast, n):
    _, depth, columns = slow.shape
    return pl.pallas_call(
        functools.partial(first_kernel, n),
        out_shape=[jax.ShapeDtypeStruct((depth, columns), jnp.float32)] * STREAMS,
        in_specs=[SMEM, HBM, HBM],
        out_specs=[VMEM] * STREAMS,
        scratch_shapes=[
            pltpu.VMEM((STREAMS, depth, columns), jnp.float32),
            pltpu.VMEM((STREAMS, depth, columns), jnp.bfloat16),
            pltpu.SemaphoreType.DMA((2, STREAMS)),
        ],
        cost_estimate=estimate(STREAMS * depth * columns, 10, 1),
        compiler_params=grant(STREAMS * depth * columns, 10),
        name="first",
    )(place, slow, fast)


def add_kernel(n, back, s, last, place_ref, got_ref, slow_ref, fast_ref, *outs):
    index = piece_index(place_ref, n, back, s)
    value = got_ref[...] + (slow_ref[index] - fast_ref[index].astype(jnp.float32))
    outs[0][...] = value
    if last:
        mean = value * (1.0 / n)
        outs[1][...] = jnp.sum((mean * mean).reshape(-1, 8, 128), axis=0)


def add_piece(place, got, slow, fast, n, back, s, last):
    out_shape = [jax.ShapeDtypeStruct(got.shape, jnp.float32)]
    if last:
        out_shape.append(jax.ShapeDtypeStruct((8, 128), jnp.float32))
    return pl.pallas_call(
        functools.partial(add_kernel, n, back, s, last),
        out_shape=out_shape,
        in_specs=[SMEM, VMEM, VMEM, VMEM],
        out_specs=[VMEM] * len(out_shape),
        cost_estimate=estimate(got.size, 14, 2),
        compiler_params=grant(0, 4),
        name="add",
    )(place, got, slow, fast)


def update_kernel(n, backs, n_outs, place_ref, factor_ref, slow_ref, momentum_ref, *refs):
    count = len(backs)
    sums = refs[:count]
    slow_out, momentum_out, fast_out = refs[count + n_outs : count + n_outs + 3]
    slow_buf, momentum_buf, fast_buf, sems = refs[count + n_outs + 3 :]
    factor = factor_ref[0, 0]
    copies = []
    for k, (back, s) in enumerate(backs):
        index = piece_index(place_ref, n, back, s)
        gradient = factor * (sums[k][...] * (1.0 / n))
        momentum_next = MOMENTUM_RATE * momentum_ref[index] + gradient
        slow_next = slow_ref[index] - OUTER_RATE * (gradient + MOMENTUM_RATE * momentum_next)
        slow_buf[k] = slow_next
        momentum_buf[k] = momentum_next
        fast_buf[k] = slow_next.astype(jnp.bfloat16)
        for j, (buf, out) in enumerate(
            ((slow_buf, slow_out), (momentum_buf, momentum_out), (fast_buf, fast_out))
        ):
            copy = pltpu.make_async_copy(buf.at[k], out.at[index], sems.at[j, k])
            copy.start()
            copies.append(copy)
    for copy in copies:
        copy.wait()


def update(place, factor, chunks, slow, momentum, outs, n):
    backs = [(back, s) for back, s, _ in chunks]
    count = len(chunks)
    _, depth, columns = slow.shape
    return pl.pallas_call(
        functools.partial(update_kernel, n, backs, len(outs)),
        out_shape=(
            jax.ShapeDtypeStruct(slow.shape, jnp.float32),
            jax.ShapeDtypeStruct(slow.shape, jnp.float32),
            jax.ShapeDtypeStruct(slow.shape, jnp.bfloat16),
        ),
        in_specs=[SMEM, SMEM, VMEM, VMEM] + [VMEM] * count + [HBM] * len(outs),
        out_specs=(HBM, HBM, HBM),
        scratch_shapes=[
            pltpu.VMEM((count, depth, columns), jnp.float32),
            pltpu.VMEM((count, depth, columns), jnp.float32),
            pltpu.VMEM((count, depth, columns), jnp.bfloat16),
            pltpu.SemaphoreType.DMA((3, count)),
        ],
        input_output_aliases={4 + count + k: k for k in range(len(outs))},
        cost_estimate=estimate(count * depth * columns, 22, 8),
        compiler_params=grant(count * depth * columns, 14),
        name="update",
    )(place, factor, slow, momentum, *[sums for _, _, sums in chunks], *outs)


def ring_perm(n, m):
    order = [2 * k for k in range(n // 2)] + [n - 1 - 2 * k for k in range(n // 2)]
    if n % 2:
        order = list(range(n))
    perm = []
    for k in range(n):
        for c in range(m):
            other = (k + 1) % n if c % 2 == 0 else (k - 1) % n
            perm.append((order[k] * m + c, order[other] * m + c))
    return perm


def total_over_all(value, n, m):
    if n & (n - 1) or m & (m - 1):
        return lax.psum(value, ("dp", "mp"))
    bit = 1
    while bit < m:
        value = value + lax.ppermute(value, "mp", [(i, i ^ bit) for i in range(m)])
        bit *= 2
    bit = 1
    while bit < n:
        value = value + lax.ppermute(value, "dp", [(i, i ^ bit) for i in range(n)])
        bit *= 2
    return value


def body(slow_weights, fast_weights, momentum):
    n, m = lax.axis_size("dp"), lax.axis_size("mp")
    rows, columns = slow_weights.shape[1:]
    max_norm = CLIP_LEVEL * math.sqrt(slow_weights.size * m)
    depth = rows // (n * STREAMS)
    slow = slow_weights.reshape(n * STREAMS, depth, columns)
    fast = fast_weights.reshape(n * STREAMS, depth, columns)
    moment = momentum.reshape(n * STREAMS, depth, columns)

    me = lax.axis_index("dp")
    position = me if n % 2 else jnp.where(me % 2 == 0, me // 2, n - 1 - me // 2)
    way = jnp.where(lax.axis_index("mp") % 2 == 0, -1, 1)
    place = jnp.stack([position, way]).astype(jnp.int32)
    perm = ring_perm(n, m)

    def hop(value):
        return lax.ppermute(value, ("dp", "mp"), perm)

    held = list(first_pieces(place, slow, fast, n))
    squares = [None] * STREAMS
    for step in range(n - 1):
        for s in range(STREAMS):
            last = step == n - 2
            out = add_piece(place, hop(held[s]), slow, fast, n, step + 2, s, last)
            held[s] = out[0]
            if last:
                squares[s] = out[1]

    chunks = [(0, s, held[s]) for s in range(STREAMS)]
    for step in range(n - 1):
        for s in range(STREAMS):
            held[s] = hop(held[s])
            chunks.append((step + 1, s, held[s]))

    norm = jnp.sqrt(jnp.sum(total_over_all(sum(squares), n, m)))
    factor = jnp.minimum(1.0, max_norm / (norm + EPSILON)).reshape(1, 1)

    cut = len(chunks) - STREAMS
    outs = update(place, factor, chunks[:cut], slow, moment, (), n)
    outs = update(place, factor, chunks[cut:], slow, moment, outs, n)
    slow_next, momentum_next, fast_next = outs
    return (
        slow_next.reshape(slow_weights.shape),
        momentum_next.reshape(momentum.shape),
        fast_next.reshape(fast_weights.shape),
    )


def solution(mesh):
    in_specs = (P(None, None, "mp"), P("dp", None, None, "mp"), P(None, None, "mp"))
    out_specs = (P(None, None, "mp"), P(None, None, "mp"), P("dp", None, None, "mp"))
    return jax.shard_map(body, mesh=mesh, in_specs=in_specs, out_specs=out_specs, check_vma=False)
```

```python
import functools
import math

import jax
import jax.numpy as jnp
from jax import lax
from jax.experimental import pallas as pl
from jax.experimental.pallas import tpu as pltpu
from jax.sharding import PartitionSpec as P


MOMENTUM_RATE = 0.9
OUTER_RATE = 0.7
CLIP_LEVEL = 0.2
EPSILON = 1e-06
STREAMS = 4
GAP = 4
LATE = 2
VMEM = pl.BlockSpec(memory_space=pltpu.VMEM)
SMEM = pl.BlockSpec(memory_space=pltpu.SMEM)
HBM = pl.BlockSpec(memory_space=pltpu.HBM)


def split(rows, tile=8):
    tiles = rows // tile
    edges = [tile * (tiles * s // STREAMS) for s in range(STREAMS)] + [rows]
    return [(a, b - a) for a, b in zip(edges[:-1], edges[1:])]


def chunk_index(n, back):
    me = lax.axis_index("dp")
    way = 2 * lax.rem(lax.axis_index("mp"), 2) - 1
    if n % 2:
        place = me
    else:
        half = lax.div(me, 2)
        place = jnp.where(lax.rem(me, 2) == 0, half, n - 1 - half)
    return lax.rem(place + way * back + 2 * n, n)


def estimate(elements, bytes_each, flops_each):
    return pl.CostEstimate(
        flops=flops_each * elements, bytes_accessed=bytes_each * elements, transcendentals=0
    )


def grant(byte_count):
    return pltpu.CompilerParams(vmem_limit_bytes=byte_count + (1 << 20))


def first_kernel(n, start, rows, slow_ref, fast_ref, out_ref, slow_buf, fast_buf, sems):
    here = (chunk_index(n, 1), pl.ds(start, rows))
    a = pltpu.make_async_copy(slow_ref.at[here], slow_buf, sems.at[0])
    b = pltpu.make_async_copy(fast_ref.at[here], fast_buf, sems.at[1])
    a.start()
    b.start()
    a.wait()
    b.wait()
    out_ref[...] = slow_buf[...] - fast_buf[...].astype(jnp.float32)


def first_piece(slow, fast, n, part):
    columns = slow.shape[2]
    rows = part[1]
    slow = pltpu.with_memory_space_constraint(slow, pltpu.HBM)
    fast = pltpu.with_memory_space_constraint(fast, pltpu.HBM)
    return pl.pallas_call(
        functools.partial(first_kernel, n, *part),
        out_shape=jax.ShapeDtypeStruct((rows, columns), jnp.float32),
        in_specs=[HBM, HBM],
        out_specs=VMEM,
        scratch_shapes=[
            pltpu.VMEM((rows, columns), jnp.float32),
            pltpu.VMEM((rows, columns), jnp.bfloat16),
            pltpu.SemaphoreType.DMA((2,)),
        ],
        cost_estimate=estimate(rows * columns, 10, 1),
        compiler_params=grant(rows * columns * 6),
        name="first",
    )(slow, fast)


def own_kernel(n, start, rows, slow_ref, fast_ref, out_ref):
    here = (chunk_index(n, 1), pl.ds(start, rows))
    out_ref[...] = slow_ref[here] - fast_ref[here].astype(jnp.float32)


def own_piece(slow, fast, n, part):
    shape = (part[1], slow.shape[2])
    return pl.pallas_call(
        functools.partial(own_kernel, n, *part),
        out_shape=jax.ShapeDtypeStruct(shape, jnp.float32),
        in_specs=[VMEM, VMEM],
        out_specs=VMEM,
        cost_estimate=estimate(shape[0] * shape[1], 10, 1),
        compiler_params=grant(0),
        name="own",
    )(slow, fast)


def add_kernel(n, back, start, rows, got_ref, slow_ref, fast_ref, *refs):
    here = (chunk_index(n, back), pl.ds(start, rows))
    refs[-1][...] = got_ref[...] + (slow_ref[here] - fast_ref[here].astype(jnp.float32))


def add_piece(got, state, n, back, part):
    return pl.pallas_call(
        functools.partial(add_kernel, n, back, *part),
        out_shape=jax.ShapeDtypeStruct(got.shape, jnp.float32),
        in_specs=[VMEM] * (1 + len(state)),
        out_specs=VMEM,
        cost_estimate=estimate(got.size, 160, 2),
        compiler_params=grant(0),
        name="add",
    )(got, *state)


def tally_kernel(n, chunks, *refs):
    out = refs[-1]
    place = lax.broadcasted_iota(jnp.int32, out.shape, 0)
    table = jnp.zeros(out.shape, jnp.float32)
    for back, positions in chunks:
        squares = jnp.zeros((8, 128), jnp.float32)
        for k in positions:
            mean = refs[k][...] * (1.0 / n)
            squares = squares + jnp.sum((mean * mean).reshape(-1, 8, 128), axis=0)
        row = jnp.sum(squares, axis=0, keepdims=True)
        table = jnp.where(place == chunk_index(n, back), row, table)
    out[...] = table


def tally(chunks, state, n):
    pieces = [piece for chunk in chunks for piece in chunk]
    count = len(chunks[0])
    spans = [(chunk[0][0], range(count * k, count * (k + 1))) for k, chunk in enumerate(chunks)]
    values = [sums for _, _, sums in pieces]
    return pl.pallas_call(
        functools.partial(tally_kernel, n, spans),
        out_shape=jax.ShapeDtypeStruct((-(-n // 8) * 8, 128), jnp.float32),
        in_specs=[VMEM] * (len(values) + len(state)),
        out_specs=VMEM,
        cost_estimate=estimate(sum(v.size for v in values), 40, 3),
        compiler_params=grant(0),
        name="tally",
    )(*values, *state)


def sum_kernel(*refs):
    refs[-1][...] = refs[0][...] + refs[1][...]


def sum_small(a, b, state):
    return pl.pallas_call(
        sum_kernel,
        out_shape=jax.ShapeDtypeStruct(a.shape, jnp.float32),
        in_specs=[VMEM] * (2 + len(state)),
        out_specs=VMEM,
        cost_estimate=estimate(a.size, 12, 1),
        compiler_params=grant(0),
        name="sum",
    )(a, b, *state)


def update_kernel(n, max_norm, pieces, n_outs, total_ref, slow_ref, momentum_ref, *refs):
    count = len(pieces)
    sums = refs[:count]
    slow_out, momentum_out, fast_out = refs[count + n_outs : count + n_outs + 3]
    slow_buf, momentum_buf, fast_buf, sems = refs[count + n_outs + 3 :]
    norm = jnp.sqrt(jnp.sum(total_ref[...], keepdims=True))
    factor = jnp.minimum(1.0, max_norm / (norm + EPSILON))
    copies = []
    at = 0
    for k, (back, start, rows) in enumerate(pieces):
        index = chunk_index(n, back)
        here, there = pl.ds(start, rows), pl.ds(at, rows)
        gradient = factor * (sums[k][...] * (1.0 / n))
        momentum_next = MOMENTUM_RATE * momentum_ref[index, here] + gradient
        slow_next = slow_ref[index, here] - OUTER_RATE * (gradient + MOMENTUM_RATE * momentum_next)
        slow_buf[there] = slow_next
        momentum_buf[there] = momentum_next
        fast_buf[there] = slow_next.astype(jnp.bfloat16)
        for j, (buf, out) in enumerate(
            ((slow_buf, slow_out), (momentum_buf, momentum_out), (fast_buf, fast_out))
        ):
            copy = pltpu.make_async_copy(buf.at[there], out.at[index, here], sems.at[j, k])
            copy.start()
            copies.append(copy)
        at += rows
    for copy in copies:
        copy.wait()


def update(total, chunks, slow, momentum, outs, n, max_norm):
    pieces = [(back, start, rows) for back, (start, rows), _ in chunks]
    count = len(chunks)
    columns = slow.shape[2]
    rows = sum(rows for _, _, rows in pieces)
    return pl.pallas_call(
        functools.partial(update_kernel, n, max_norm, pieces, len(outs)),
        out_shape=(
            pltpu.HBM(slow.shape, jnp.float32),
            pltpu.HBM(slow.shape, jnp.float32),
            pltpu.HBM(slow.shape, jnp.bfloat16),
        ),
        in_specs=[VMEM, VMEM, VMEM] + [VMEM] * count + [HBM] * len(outs),
        out_specs=(HBM, HBM, HBM),
        scratch_shapes=[
            pltpu.VMEM((rows, columns), jnp.float32),
            pltpu.VMEM((rows, columns), jnp.float32),
            pltpu.VMEM((rows, columns), jnp.bfloat16),
            pltpu.SemaphoreType.DMA((3, count)),
        ],
        input_output_aliases={3 + count + k: k for k in range(len(outs))},
        cost_estimate=estimate(rows * columns, 22, 8),
        compiler_params=grant(rows * columns * 15),
        name="update",
    )(total, slow, momentum, *[sums for _, _, sums in chunks], *outs)


def ring_order(n):
    if n % 2:
        return list(range(n))
    return [2 * k for k in range(n // 2)] + [n - 1 - 2 * k for k in range(n // 2)]


def ring_perm(n, m):
    order = ring_order(n)
    perm = []
    for k in range(n):
        for c in range(m):
            other = (k + 1) % n if c % 2 == 0 else (k - 1) % n
            perm.append((order[k] * m + c, order[other] * m + c))
    return perm


def exchanges(n, m):
    order = ring_order(n)
    across = None if n % 2 else [(order[k], order[(k + n // 2) % n]) for k in range(n)]
    steps = [("dp", across)]
    if m & (m - 1):
        return steps + [("mp", None)]
    bit = 1
    while bit < m:
        steps.append(("mp", [(i, i ^ bit) for i in range(m)]))
        bit *= 2
    return steps


def exchange_slots(n, m):
    count = len(exchanges(n, m))
    return [STREAMS * (n - 1) - GAP * (count - j) for j in range(count)]


def body(slow_weights, fast_weights, momentum):
    n, m = lax.axis_size("dp"), lax.axis_size("mp")
    rows, columns = slow_weights.shape[1:]
    max_norm = CLIP_LEVEL * math.sqrt(slow_weights.size * m)
    depth = rows // n
    slow = slow_weights.reshape(n, depth, columns)
    fast = fast_weights.reshape(n, depth, columns)
    moment = momentum.reshape(n, depth, columns)
    parts = split(depth)
    perm = ring_perm(n, m)
    steps, slots = exchanges(n, m), exchange_slots(n, m)

    def hop(value):
        return lax.ppermute(value, ("dp", "mp"), perm)

    held = [first_piece(slow, fast, n, parts[0])]
    held += [own_piece(slow, fast, n, part) for part in parts[1:]]
    for step in range(n - 1):
        state = (slow, fast) if step < LATE else (slow, fast, moment)
        for s, part in enumerate(parts):
            held[s] = add_piece(hop(held[s]), state, n, step + 2, part)

    state = (slow, moment)
    chunks = [[(0, part, held[s]) for s, part in enumerate(parts)]]
    table, arriving = None, None
    for slot in range(STREAMS * (n - 1)):
        step, s = divmod(slot, STREAMS)
        if slot in slots:
            j = slots.index(slot)
            if j == 0:
                known = 1 if n % 2 else n // 2
                table = tally(chunks[:known], state, n)
            else:
                table = sum_small(table, arriving, state)
            axis, pairs = steps[j]
            if pairs is None:
                arriving = lax.psum(table, axis) - table
            else:
                arriving = lax.ppermute(table, axis, pairs)
        held[s] = hop(held[s])
        if s == 0:
            chunks.append([])
        chunks[-1].append((step + 1, parts[s], held[s]))
    table = sum_small(table, arriving, state)

    mine = [piece for chunk in chunks[:-1] for piece in chunk]
    outs = update(table, mine, slow, moment, (), n, max_norm)
    outs = update(table, chunks[-1], slow, moment, outs, n, max_norm)
    slow_next, momentum_next, fast_next = outs
    return (
        slow_next.reshape(slow_weights.shape),
        momentum_next.reshape(momentum.shape),
        fast_next.reshape(fast_weights.shape),
    )


def solution(mesh):
    in_specs = (P(None, None, "mp"), P("dp", None, None, "mp"), P(None, None, "mp"))
    out_specs = (P(None, None, "mp"), P(None, None, "mp"), P("dp", None, None, "mp"))
    return jax.shard_map(body, mesh=mesh, in_specs=in_specs, out_specs=out_specs, check_vma=False)
```

```python
import functools
import math

import jax
import jax.numpy as jnp
from jax import lax
from jax.experimental import pallas as pl
from jax.experimental.pallas import tpu as pltpu
from jax.sharding import PartitionSpec as P


MOMENTUM_RATE = 0.9
OUTER_RATE = 0.7
CLIP_LEVEL = 0.2
EPSILON = 1e-06
STREAMS = 4
RIDER = 2
LATE = 2
VMEM = pl.BlockSpec(memory_space=pltpu.VMEM)
SMEM = pl.BlockSpec(memory_space=pltpu.SMEM)
HBM = pl.BlockSpec(memory_space=pltpu.HBM)


def split(rows, tile=8):
    tiles = rows // tile
    edges = [tile * (tiles * s // STREAMS) for s in range(STREAMS)] + [rows]
    return [(a, b - a) for a, b in zip(edges[:-1], edges[1:])]


def chunk_index(n, back):
    me = lax.axis_index("dp")
    way = 2 * lax.rem(lax.axis_index("mp"), 2) - 1
    if n % 2:
        place = me
    else:
        half = lax.div(me, 2)
        place = jnp.where(lax.rem(me, 2) == 0, half, n - 1 - half)
    return lax.rem(place + way * back + 2 * n, n)


def estimate(elements, bytes_each, flops_each):
    return pl.CostEstimate(
        flops=flops_each * elements, bytes_accessed=bytes_each * elements, transcendentals=0
    )


def grant(byte_count):
    return pltpu.CompilerParams(vmem_limit_bytes=byte_count + (1 << 20))


def first_kernel(n, start, rows, slow_ref, fast_ref, out_ref, slow_buf, fast_buf, sems):
    here = (chunk_index(n, 1), pl.ds(start, rows))
    a = pltpu.make_async_copy(slow_ref.at[here], slow_buf, sems.at[0])
    b = pltpu.make_async_copy(fast_ref.at[here], fast_buf, sems.at[1])
    a.start()
    b.start()
    a.wait()
    b.wait()
    out_ref[...] = slow_buf[...] - fast_buf[...].astype(jnp.float32)


def first_piece(slow, fast, n, part):
    columns = slow.shape[2]
    rows = part[1]
    slow = pltpu.with_memory_space_constraint(slow, pltpu.HBM)
    fast = pltpu.with_memory_space_constraint(fast, pltpu.HBM)
    return pl.pallas_call(
        functools.partial(first_kernel, n, *part),
        out_shape=jax.ShapeDtypeStruct((rows, columns), jnp.float32),
        in_specs=[HBM, HBM],
        out_specs=VMEM,
        scratch_shapes=[
            pltpu.VMEM((rows, columns), jnp.float32),
            pltpu.VMEM((rows, columns), jnp.bfloat16),
            pltpu.SemaphoreType.DMA((2,)),
        ],
        cost_estimate=estimate(rows * columns, 10, 1),
        compiler_params=grant(rows * columns * 6),
        name="first",
    )(slow, fast)


def own_kernel(n, start, rows, slow_ref, fast_ref, out_ref):
    here = (chunk_index(n, 1), pl.ds(start, rows))
    out_ref[...] = slow_ref[here] - fast_ref[here].astype(jnp.float32)


def own_piece(slow, fast, n, part):
    shape = (part[1], slow.shape[2])
    return pl.pallas_call(
        functools.partial(own_kernel, n, *part),
        out_shape=jax.ShapeDtypeStruct(shape, jnp.float32),
        in_specs=[VMEM, VMEM],
        out_specs=VMEM,
        cost_estimate=estimate(shape[0] * shape[1], 10, 1),
        compiler_params=grant(0),
        name="own",
    )(slow, fast)


def add_kernel(n, back, start, rows, got_ref, slow_ref, fast_ref, *refs):
    here = (chunk_index(n, back), pl.ds(start, rows))
    refs[-1][...] = got_ref[...] + (slow_ref[here] - fast_ref[here].astype(jnp.float32))


def add_piece(got, state, n, back, part):
    return pl.pallas_call(
        functools.partial(add_kernel, n, back, *part),
        out_shape=jax.ShapeDtypeStruct(got.shape, jnp.float32),
        in_specs=[VMEM] * (1 + len(state)),
        out_specs=VMEM,
        cost_estimate=estimate(got.size, 160, 2),
        compiler_params=grant(0),
        name="add",
    )(got, *state)


def tally_kernel(n, count, *refs):
    out = refs[-1]
    squares = jnp.zeros((8, 128), jnp.float32)
    for ref in refs[:count]:
        mean = ref[...] * (1.0 / n)
        squares = squares + jnp.sum((mean * mean).reshape(-1, 8, 128), axis=0)
    row = jnp.sum(squares, axis=0, keepdims=True)
    lane = 128 * lax.rem(lax.axis_index("mp"), 2)
    place = lax.broadcasted_iota(jnp.int32, (out.shape[0], 128), 0)
    out[...] = jnp.zeros_like(out)
    out[:, pl.ds(pl.multiple_of(lane, 128), 128)] = jnp.where(place == chunk_index(n, 0), row, 0.0)


def tally(values, state, n):
    columns = values[0].shape[1]
    return pl.pallas_call(
        functools.partial(tally_kernel, n, len(values)),
        out_shape=jax.ShapeDtypeStruct((-(-n // 8) * 8, columns), jnp.float32),
        in_specs=[VMEM] * (len(values) + len(state)),
        out_specs=VMEM,
        cost_estimate=estimate(sum(v.size for v in values), 40, 3),
        compiler_params=grant(0),
        name="tally",
    )(*values, *state)


def merge_kernel(how, count, *refs):
    table = refs[0][...]
    for ref in refs[1:count]:
        other = ref[ref.shape[0] - table.shape[0] :, :]
        table = table + other if how == "sum" else jnp.maximum(table, other)
    refs[-1][...] = table


def merge(tables, state, how):
    return pl.pallas_call(
        functools.partial(merge_kernel, how, len(tables)),
        out_shape=jax.ShapeDtypeStruct(tables[0].shape, jnp.float32),
        in_specs=[VMEM] * (len(tables) + len(state)),
        out_specs=VMEM,
        cost_estimate=estimate(tables[0].size, 12, 1),
        compiler_params=grant(0),
        name="merge",
    )(*tables, *state)


def load_kernel(piece_ref, table_ref, other_ref, *refs):
    out = refs[-1]
    rows = piece_ref.shape[0]
    out[:rows, :] = piece_ref[...]
    out[rows:, :] = jnp.maximum(table_ref[...], other_ref[...])


def load_rider(piece, table, other, state):
    shape = (piece.shape[0] + table.shape[0], piece.shape[1])
    return pl.pallas_call(
        load_kernel,
        out_shape=jax.ShapeDtypeStruct(shape, jnp.float32),
        in_specs=[VMEM] * (3 + len(state)),
        out_specs=VMEM,
        cost_estimate=estimate(piece.size, 12, 1),
        compiler_params=grant(0),
        name="load",
    )(piece, table, other, *state)


def update_kernel(n, max_norm, pieces, n_outs, total_ref, slow_ref, momentum_ref, *refs):
    count = len(pieces)
    sums = refs[:count]
    slow_out, momentum_out, fast_out = refs[count + n_outs : count + n_outs + 3]
    slow_buf, momentum_buf, fast_buf, sems = refs[count + n_outs + 3 :]
    norm = jnp.sqrt(jnp.sum(total_ref[...], keepdims=True))
    factor = jnp.minimum(1.0, max_norm / (norm + EPSILON))
    copies = []
    at = 0
    for k, (back, start, rows) in enumerate(pieces):
        index = chunk_index(n, back)
        here, there = pl.ds(start, rows), pl.ds(at, rows)
        gradient = factor * (sums[k][:rows, :] * (1.0 / n))
        momentum_next = MOMENTUM_RATE * momentum_ref[index, here] + gradient
        slow_next = slow_ref[index, here] - OUTER_RATE * (gradient + MOMENTUM_RATE * momentum_next)
        slow_buf[there] = slow_next
        momentum_buf[there] = momentum_next
        fast_buf[there] = slow_next.astype(jnp.bfloat16)
        for j, (buf, out) in enumerate(
            ((slow_buf, slow_out), (momentum_buf, momentum_out), (fast_buf, fast_out))
        ):
            copy = pltpu.make_async_copy(buf.at[there], out.at[index, here], sems.at[j, k])
            copy.start()
            copies.append(copy)
        at += rows
    for copy in copies:
        copy.wait()


def update(total, chunks, slow, momentum, outs, n, max_norm):
    pieces = [(back, start, rows) for back, (start, rows), _ in chunks]
    count = len(chunks)
    columns = slow.shape[2]
    rows = sum(rows for _, _, rows in pieces)
    return pl.pallas_call(
        functools.partial(update_kernel, n, max_norm, pieces, len(outs)),
        out_shape=(
            pltpu.HBM(slow.shape, jnp.float32),
            pltpu.HBM(slow.shape, jnp.float32),
            pltpu.HBM(slow.shape, jnp.bfloat16),
        ),
        in_specs=[VMEM, VMEM, VMEM] + [VMEM] * count + [HBM] * len(outs),
        out_specs=(HBM, HBM, HBM),
        scratch_shapes=[
            pltpu.VMEM((rows, columns), jnp.float32),
            pltpu.VMEM((rows, columns), jnp.float32),
            pltpu.VMEM((rows, columns), jnp.bfloat16),
            pltpu.SemaphoreType.DMA((3, count)),
        ],
        input_output_aliases={3 + count + k: k for k in range(len(outs))},
        cost_estimate=estimate(rows * columns, 22, 8),
        compiler_params=grant(rows * columns * 15),
        name="update",
    )(total, slow, momentum, *[sums for _, _, sums in chunks], *outs)


def ring_order(n):
    if n % 2:
        return list(range(n))
    return [2 * k for k in range(n // 2)] + [n - 1 - 2 * k for k in range(n // 2)]


def ring_perm(n, m):
    order = ring_order(n)
    perm = []
    for k in range(n):
        for c in range(m):
            other = (k + 1) % n if c % 2 == 0 else (k - 1) % n
            perm.append((order[k] * m + c, order[other] * m + c))
    return perm


def rides(n, m):
    return n % 2 == 0 and m > 1 and m & (m - 1) == 0


def exchanges(n, m):
    hops = STREAMS * (n - 1)
    arrived = STREAMS * (1 + n // 2) + RIDER
    swap = [(c, c ^ 1) for c in range(m)]
    steps = [(swap, STREAMS, STREAMS + RIDER), (swap, arrived + 1, arrived + 3)]
    bit = 2
    while bit < m:
        start = steps[-1][2]
        steps.append(([(c, c ^ bit) for c in range(m)], start, min(start + STREAMS - 1, hops)))
        bit *= 2
    return steps


def body(slow_weights, fast_weights, momentum):
    n, m = lax.axis_size("dp"), lax.axis_size("mp")
    rows, columns = slow_weights.shape[1:]
    max_norm = CLIP_LEVEL * math.sqrt(slow_weights.size * m)
    depth = rows // n
    slow = slow_weights.reshape(n, depth, columns)
    fast = fast_weights.reshape(n, depth, columns)
    moment = momentum.reshape(n, depth, columns)
    parts = split(depth)
    perm = ring_perm(n, m)
    riding = rides(n, m)
    steps = exchanges(n, m) if riding else []

    def hop(value):
        return lax.ppermute(value, ("dp", "mp"), perm)

    held = [first_piece(slow, fast, n, parts[0])]
    held += [own_piece(slow, fast, n, part) for part in parts[1:]]
    for step in range(n - 1):
        state = (slow, fast) if step < LATE else (slow, fast, moment)
        for s, part in enumerate(parts):
            held[s] = add_piece(hop(held[s]), state, n, step + 2, part)

    state = (slow, moment)
    chunks = [[(0, part, held[s]) for s, part in enumerate(parts)]]
    table = tally([sums for _, _, sums in chunks[0]], state, n)
    if not riding:
        table = lax.psum(table, ("dp", "mp"))
    got = [None] * len(steps)

    def swap(j, value):
        return lax.ppermute(value, "mp", steps[j][0])

    for slot in range(STREAMS * (n - 1) + 1):
        step, s = divmod(slot, STREAMS)
        for j, (_, start, end) in enumerate(steps):
            if slot == end and j == 0:
                held[s] = load_rider(held[s], table, got[j], state)
            elif slot == end:
                table = merge([table, got[j]], state, "max" if j == 1 else "sum")
            if slot == start:
                if j == 1:
                    riders = [chunk[RIDER][2] for chunk in chunks[2 : 2 + n // 2]]
                    table = merge([table, got[0]] + riders, state, "max")
                got[j] = swap(j, table)
        if step == n - 1:
            break
        held[s] = hop(held[s])
        if s == 0:
            chunks.append([])
        chunks[-1].append((step + 1, parts[s], held[s]))

    mine = [piece for chunk in chunks[:-1] for piece in chunk]
    outs = update(table, mine, slow, moment, (), n, max_norm)
    outs = update(table, chunks[-1], slow, moment, outs, n, max_norm)
    slow_next, momentum_next, fast_next = outs
    return (
        slow_next.reshape(slow_weights.shape),
        momentum_next.reshape(momentum.shape),
        fast_next.reshape(fast_weights.shape),
    )


def solution(mesh):
    in_specs = (P(None, None, "mp"), P("dp", None, None, "mp"), P(None, None, "mp"))
    out_specs = (P(None, None, "mp"), P(None, None, "mp"), P("dp", None, None, "mp"))
    return jax.shard_map(body, mesh=mesh, in_specs=in_specs, out_specs=out_specs, check_vma=False)
```

```python
import functools
import math

import jax
import jax.numpy as jnp
from jax import lax
from jax.experimental import pallas as pl
from jax.experimental.pallas import tpu as pltpu
from jax.sharding import PartitionSpec as P


MOMENTUM_RATE = 0.9
OUTER_RATE = 0.7
CLIP_LEVEL = 0.2
EPSILON = 1e-06
STREAMS = 4
RIDER = 1
FIRST = 2
LATE = 2
VMEM = pl.BlockSpec(memory_space=pltpu.VMEM)
SMEM = pl.BlockSpec(memory_space=pltpu.SMEM)
HBM = pl.BlockSpec(memory_space=pltpu.HBM)


def split(rows, tile=8):
    tiles = rows // tile
    edges = [tile * (tiles * s // STREAMS) for s in range(STREAMS)] + [rows]
    return [(a, b - a) for a, b in zip(edges[:-1], edges[1:])]


def chunk_index(n, back):
    me = lax.axis_index("dp")
    way = 2 * lax.rem(lax.axis_index("mp"), 2) - 1
    if n % 2:
        place = me
    else:
        half = lax.div(me, 2)
        place = jnp.where(lax.rem(me, 2) == 0, half, n - 1 - half)
    return lax.rem(place + way * back + 2 * n, n)


def estimate(elements, bytes_each, flops_each):
    return pl.CostEstimate(
        flops=flops_each * elements, bytes_accessed=bytes_each * elements, transcendentals=0
    )


def grant(byte_count):
    return pltpu.CompilerParams(vmem_limit_bytes=byte_count + (1 << 20))


def first_kernel(n, parts, slow_ref, fast_ref, *refs):
    outs, (slow_buf, fast_buf, sems) = refs[: len(parts)], refs[len(parts) :]
    index = chunk_index(n, 1)
    copies = []
    for s, (start, rows) in enumerate(parts):
        here = pl.ds(start, rows)
        a = pltpu.make_async_copy(slow_ref.at[index, here], slow_buf.at[here], sems.at[0, s])
        b = pltpu.make_async_copy(fast_ref.at[index, here], fast_buf.at[here], sems.at[1, s])
        a.start()
        b.start()
        copies.append((a, b))
    for s, (start, rows) in enumerate(parts):
        here = pl.ds(start, rows)
        for copy in copies[s]:
            copy.wait()
        outs[s][...] = slow_buf[here] - fast_buf[here].astype(jnp.float32)


def first_pieces(slow, fast, n, parts):
    columns = slow.shape[2]
    depth = parts[-1][0] + parts[-1][1]
    slow = pltpu.with_memory_space_constraint(slow, pltpu.HBM)
    fast = pltpu.with_memory_space_constraint(fast, pltpu.HBM)
    return pl.pallas_call(
        functools.partial(first_kernel, n, parts),
        out_shape=[jax.ShapeDtypeStruct((rows, columns), jnp.float32) for _, rows in parts],
        in_specs=[HBM, HBM],
        out_specs=[VMEM] * len(parts),
        scratch_shapes=[
            pltpu.VMEM((depth, columns), jnp.float32),
            pltpu.VMEM((depth, columns), jnp.bfloat16),
            pltpu.SemaphoreType.DMA((2, len(parts))),
        ],
        cost_estimate=estimate(depth * columns, 10, 1),
        compiler_params=grant(depth * columns * 6),
        name="first",
    )(slow, fast)


def own_kernel(n, start, rows, slow_ref, fast_ref, out_ref):
    here = (chunk_index(n, 1), pl.ds(start, rows))
    out_ref[...] = slow_ref[here] - fast_ref[here].astype(jnp.float32)


def own_piece(slow, fast, n, part):
    shape = (part[1], slow.shape[2])
    return pl.pallas_call(
        functools.partial(own_kernel, n, *part),
        out_shape=jax.ShapeDtypeStruct(shape, jnp.float32),
        in_specs=[VMEM, VMEM],
        out_specs=VMEM,
        cost_estimate=estimate(shape[0] * shape[1], 10, 1),
        compiler_params=grant(0),
        name="own",
    )(slow, fast)


def add_kernel(n, back, start, rows, got_ref, slow_ref, fast_ref, *refs):
    here = (chunk_index(n, back), pl.ds(start, rows))
    refs[-1][...] = got_ref[...] + (slow_ref[here] - fast_ref[here].astype(jnp.float32))


def add_piece(got, state, n, back, part):
    return pl.pallas_call(
        functools.partial(add_kernel, n, back, *part),
        out_shape=jax.ShapeDtypeStruct(got.shape, jnp.float32),
        in_specs=[VMEM] * (1 + len(state)),
        out_specs=VMEM,
        cost_estimate=estimate(got.size, 160, 2),
        compiler_params=grant(0),
        name="add",
    )(got, *state)


def tally_kernel(n, count, *refs):
    out = refs[-1]
    squares = jnp.zeros((8, 128), jnp.float32)
    for ref in refs[:count]:
        mean = ref[...] * (1.0 / n)
        squares = squares + jnp.sum((mean * mean).reshape(-1, 8, 128), axis=0)
    row = jnp.sum(squares, axis=0, keepdims=True)
    lane = 128 * lax.rem(lax.axis_index("mp"), 2)
    place = lax.broadcasted_iota(jnp.int32, (out.shape[0], 128), 0)
    out[...] = jnp.zeros_like(out)
    out[:, pl.ds(pl.multiple_of(lane, 128), 128)] = jnp.where(place == chunk_index(n, 0), row, 0.0)


def tally(values, state, n):
    columns = values[0].shape[1]
    return pl.pallas_call(
        functools.partial(tally_kernel, n, len(values)),
        out_shape=jax.ShapeDtypeStruct((-(-n // 8) * 8, columns), jnp.float32),
        in_specs=[VMEM] * (len(values) + len(state)),
        out_specs=VMEM,
        cost_estimate=estimate(sum(v.size for v in values), 40, 3),
        compiler_params=grant(0),
        name="tally",
    )(*values, *state)


def merge_kernel(how, count, *refs):
    table = refs[0][...]
    for ref in refs[1:count]:
        other = ref[ref.shape[0] - table.shape[0] :, :]
        table = table + other if how == "sum" else jnp.maximum(table, other)
    refs[-1][...] = table


def merge(tables, state, how):
    return pl.pallas_call(
        functools.partial(merge_kernel, how, len(tables)),
        out_shape=jax.ShapeDtypeStruct(tables[0].shape, jnp.float32),
        in_specs=[VMEM] * (len(tables) + len(state)),
        out_specs=VMEM,
        cost_estimate=estimate(tables[0].size, 12, 1),
        compiler_params=grant(0),
        name="merge",
    )(*tables, *state)


def load_kernel(piece_ref, table_ref, other_ref, *refs):
    out = refs[-1]
    rows = piece_ref.shape[0]
    out[:rows, :] = piece_ref[...]
    out[rows:, :] = jnp.maximum(table_ref[...], other_ref[...])


def load_rider(piece, table, other, state):
    shape = (piece.shape[0] + table.shape[0], piece.shape[1])
    return pl.pallas_call(
        load_kernel,
        out_shape=jax.ShapeDtypeStruct(shape, jnp.float32),
        in_specs=[VMEM] * (3 + len(state)),
        out_specs=VMEM,
        cost_estimate=estimate(piece.size, 12, 1),
        compiler_params=grant(0),
        name="load",
    )(piece, table, other, *state)


def unload_kernel(loaded_ref, *refs):
    refs[-1][...] = loaded_ref[: refs[-1].shape[0], :]


def unload_rider(loaded, rows, state):
    return pl.pallas_call(
        unload_kernel,
        out_shape=jax.ShapeDtypeStruct((rows, loaded.shape[1]), jnp.float32),
        in_specs=[VMEM] * (1 + len(state)),
        out_specs=VMEM,
        cost_estimate=estimate(loaded.size, 12, 1),
        compiler_params=grant(0),
        name="unload",
    )(loaded, *state)


def scale_kernel(max_norm, table_ref, *refs):
    norm = jnp.sqrt(jnp.sum(table_ref[...], keepdims=True))
    factor = jnp.minimum(1.0, max_norm / (norm + EPSILON))
    refs[-1][...] = jnp.broadcast_to(factor, refs[-1].shape)


def clip_factor(table, state, max_norm):
    return pl.pallas_call(
        functools.partial(scale_kernel, max_norm),
        out_shape=jax.ShapeDtypeStruct((8, table.shape[1]), jnp.float32),
        in_specs=[VMEM] * (1 + len(state)),
        out_specs=VMEM,
        cost_estimate=estimate(table.size, 12, 1),
        compiler_params=grant(0),
        name="scale",
    )(table, *state)


def update_kernel(n, pieces, n_outs, factor_ref, slow_ref, momentum_ref, *refs):
    count = len(pieces)
    sums = refs[:count]
    slow_out, momentum_out, fast_out = refs[count + n_outs : count + n_outs + 3]
    slow_buf, momentum_buf, fast_buf, sems = refs[count + n_outs + 3 :]
    factor = factor_ref[:1, :]
    copies = []
    at = 0
    for k, (back, start, rows) in enumerate(pieces):
        index = chunk_index(n, back)
        here, there = pl.ds(start, rows), pl.ds(at, rows)
        gradient = factor * (sums[k][:rows, :] * (1.0 / n))
        momentum_next = MOMENTUM_RATE * momentum_ref[index, here] + gradient
        slow_next = slow_ref[index, here] - OUTER_RATE * (gradient + MOMENTUM_RATE * momentum_next)
        slow_buf[there] = slow_next
        momentum_buf[there] = momentum_next
        fast_buf[there] = slow_next.astype(jnp.bfloat16)
        for j, (buf, out) in enumerate(
            ((slow_buf, slow_out), (momentum_buf, momentum_out), (fast_buf, fast_out))
        ):
            copy = pltpu.make_async_copy(buf.at[there], out.at[index, here], sems.at[j, k])
            copy.start()
            copies.append(copy)
        at += rows
    for copy in copies:
        copy.wait()


def update(factor, chunks, slow, momentum, outs, n):
    pieces = [(back, start, rows) for back, (start, rows), _ in chunks]
    count = len(chunks)
    columns = slow.shape[2]
    rows = sum(rows for _, _, rows in pieces)
    return pl.pallas_call(
        functools.partial(update_kernel, n, pieces, len(outs)),
        out_shape=(
            pltpu.HBM(slow.shape, jnp.float32),
            pltpu.HBM(slow.shape, jnp.float32),
            pltpu.HBM(slow.shape, jnp.bfloat16),
        ),
        in_specs=[VMEM, VMEM, VMEM] + [VMEM] * count + [HBM] * len(outs),
        out_specs=(HBM, HBM, HBM),
        scratch_shapes=[
            pltpu.VMEM((rows, columns), jnp.float32),
            pltpu.VMEM((rows, columns), jnp.float32),
            pltpu.VMEM((rows, columns), jnp.bfloat16),
            pltpu.SemaphoreType.DMA((3, count)),
        ],
        input_output_aliases={3 + count + k: k for k in range(len(outs))},
        cost_estimate=estimate(rows * columns, 22, 8),
        compiler_params=grant(rows * columns * 15),
        name="update",
    )(factor, slow, momentum, *[sums for _, _, sums in chunks], *outs)


def ring_order(n):
    if n % 2:
        return list(range(n))
    return [2 * k for k in range(n // 2)] + [n - 1 - 2 * k for k in range(n // 2)]


def ring_perm(n, m):
    order = ring_order(n)
    perm = []
    for k in range(n):
        for c in range(m):
            other = (k + 1) % n if c % 2 == 0 else (k - 1) % n
            perm.append((order[k] * m + c, order[other] * m + c))
    return perm


def rides(n, m):
    return n % 2 == 0 and m > 1 and m & (m - 1) == 0


def exchanges(n, m):
    hops = STREAMS * (n - 1)
    arrived = STREAMS * (1 + n // 2) + RIDER
    swap = [(c, c ^ 1) for c in range(m)]
    steps = [(swap, STREAMS, STREAMS + RIDER), (swap, arrived + 1, arrived + 3)]
    bit = 2
    while bit < m:
        start = steps[-1][2]
        steps.append(([(c, c ^ bit) for c in range(m)], start, min(start + STREAMS - 1, hops)))
        bit *= 2
    return steps


def body(slow_weights, fast_weights, momentum):
    n, m = lax.axis_size("dp"), lax.axis_size("mp")
    rows, columns = slow_weights.shape[1:]
    max_norm = CLIP_LEVEL * math.sqrt(slow_weights.size * m)
    depth = rows // n
    slow = slow_weights.reshape(n, depth, columns)
    fast = fast_weights.reshape(n, depth, columns)
    moment = momentum.reshape(n, depth, columns)
    parts = split(depth)
    perm = ring_perm(n, m)
    riding = rides(n, m)
    steps = exchanges(n, m) if riding else []

    def hop(value):
        return lax.ppermute(value, ("dp", "mp"), perm)

    held = list(first_pieces(slow, fast, n, parts[:FIRST]))
    held += [own_piece(slow, fast, n, part) for part in parts[FIRST:]]
    for step in range(n - 1):
        state = (slow, fast) if step < LATE else (slow, fast, moment)
        for s, part in enumerate(parts):
            held[s] = add_piece(hop(held[s]), state, n, step + 2, part)

    state = (slow, moment)
    chunks = [[(0, part, held[s]) for s, part in enumerate(parts)]]
    table = tally([sums for _, _, sums in chunks[0]], state, n)
    if not riding:
        table = lax.psum(table, ("dp", "mp"))
    got = [None] * len(steps)

    def swap(j, value):
        return lax.ppermute(value, "mp", steps[j][0])

    for slot in range(STREAMS * (n - 1) + 1):
        step, s = divmod(slot, STREAMS)
        for j, (_, start, end) in enumerate(steps):
            if slot == end and j == 0:
                held[s] = load_rider(held[s], table, got[j], state)
            elif slot == end:
                table = merge([table, got[j]], state, "max" if j == 1 else "sum")
            if slot == start:
                if j == 1:
                    riders = [chunk[RIDER][2] for chunk in chunks[2 : 2 + n // 2]]
                    table = merge([table, got[0]] + riders, state, "max")
                got[j] = swap(j, table)
        if step == n - 1:
            break
        if riding and s == RIDER and step == 1 + n // 2:
            held[s] = unload_rider(held[s], parts[s][1], state)
        held[s] = hop(held[s])
        if s == 0:
            chunks.append([])
        chunks[-1].append((step + 1, parts[s], held[s]))

    factor = clip_factor(table, state, max_norm)
    mine = [piece for chunk in chunks[:-1] for piece in chunk]
    outs = update(factor, mine, slow, moment, (), n)
    outs = update(factor, chunks[-1], slow, moment, outs, n)
    slow_next, momentum_next, fast_next = outs
    return (
        slow_next.reshape(slow_weights.shape),
        momentum_next.reshape(momentum.shape),
        fast_next.reshape(fast_weights.shape),
    )


def solution(mesh):
    in_specs = (P(None, None, "mp"), P("dp", None, None, "mp"), P(None, None, "mp"))
    out_specs = (P(None, None, "mp"), P(None, None, "mp"), P("dp", None, None, "mp"))
    return jax.shard_map(body, mesh=mesh, in_specs=in_specs, out_specs=out_specs, check_vma=False)
```

```python
import functools
import math

import jax
import jax.numpy as jnp
from jax import lax
from jax.experimental import pallas as pl
from jax.experimental.pallas import tpu as pltpu
from jax.sharding import PartitionSpec as P


MOMENTUM_RATE = 0.9
OUTER_RATE = 0.7
CLIP_LEVEL = 0.2
EPSILON = 1e-06
STREAMS = 4
RIDER = 1
FIRST = 2
LATE = 2
VMEM = pl.BlockSpec(memory_space=pltpu.VMEM)
SMEM = pl.BlockSpec(memory_space=pltpu.SMEM)
HBM = pl.BlockSpec(memory_space=pltpu.HBM)


def split(rows, tile=8):
    tiles = rows // tile
    edges = [tile * (tiles * s // STREAMS) for s in range(STREAMS)] + [rows]
    return [(a, b - a) for a, b in zip(edges[:-1], edges[1:])]


def chunk_index(n, back):
    me = lax.axis_index("dp")
    way = 2 * lax.rem(lax.axis_index("mp"), 2) - 1
    if n % 2:
        place = me
    else:
        half = lax.div(me, 2)
        place = jnp.where(lax.rem(me, 2) == 0, half, n - 1 - half)
    return lax.rem(place + way * back + 2 * n, n)


def estimate(elements, bytes_each, flops_each):
    return pl.CostEstimate(
        flops=flops_each * elements, bytes_accessed=bytes_each * elements, transcendentals=0
    )


def grant(byte_count):
    return pltpu.CompilerParams(vmem_limit_bytes=byte_count + (1 << 20))


def first_kernel(n, parts, slow_ref, fast_ref, *refs):
    outs, (slow_buf, fast_buf, sems) = refs[: len(parts)], refs[len(parts) :]
    index = chunk_index(n, 1)
    copies = []
    for s, (start, rows) in enumerate(parts):
        here = pl.ds(start, rows)
        a = pltpu.make_async_copy(slow_ref.at[index, here], slow_buf.at[here], sems.at[0, s])
        b = pltpu.make_async_copy(fast_ref.at[index, here], fast_buf.at[here], sems.at[1, s])
        a.start()
        b.start()
        copies.append((a, b))
    for s, (start, rows) in enumerate(parts):
        here = pl.ds(start, rows)
        for copy in copies[s]:
            copy.wait()
        outs[s][...] = slow_buf[here] - fast_buf[here].astype(jnp.float32)


def first_pieces(slow, fast, n, parts):
    columns = slow.shape[2]
    depth = parts[-1][0] + parts[-1][1]
    slow = pltpu.with_memory_space_constraint(slow, pltpu.HBM)
    fast = pltpu.with_memory_space_constraint(fast, pltpu.HBM)
    return pl.pallas_call(
        functools.partial(first_kernel, n, parts),
        out_shape=[jax.ShapeDtypeStruct((rows, columns), jnp.float32) for _, rows in parts],
        in_specs=[HBM, HBM],
        out_specs=[VMEM] * len(parts),
        scratch_shapes=[
            pltpu.VMEM((depth, columns), jnp.float32),
            pltpu.VMEM((depth, columns), jnp.bfloat16),
            pltpu.SemaphoreType.DMA((2, len(parts))),
        ],
        cost_estimate=estimate(depth * columns, 10, 1),
        compiler_params=grant(depth * columns * 6),
        name="first",
    )(slow, fast)


def own_kernel(n, start, rows, slow_ref, fast_ref, out_ref):
    here = (chunk_index(n, 1), pl.ds(start, rows))
    out_ref[...] = slow_ref[here] - fast_ref[here].astype(jnp.float32)


def own_piece(slow, fast, n, part):
    shape = (part[1], slow.shape[2])
    return pl.pallas_call(
        functools.partial(own_kernel, n, *part),
        out_shape=jax.ShapeDtypeStruct(shape, jnp.float32),
        in_specs=[VMEM, VMEM],
        out_specs=VMEM,
        cost_estimate=estimate(shape[0] * shape[1], 10, 1),
        compiler_params=grant(0),
        name="own",
    )(slow, fast)


def add_kernel(n, back, start, rows, got_ref, slow_ref, fast_ref, *refs):
    here = (chunk_index(n, back), pl.ds(start, rows))
    refs[-1][...] = got_ref[...] + (slow_ref[here] - fast_ref[here].astype(jnp.float32))


def add_piece(got, state, n, back, part):
    return pl.pallas_call(
        functools.partial(add_kernel, n, back, *part),
        out_shape=jax.ShapeDtypeStruct(got.shape, jnp.float32),
        in_specs=[VMEM] * (1 + len(state)),
        out_specs=VMEM,
        cost_estimate=estimate(got.size, 160, 2),
        compiler_params=grant(0),
        name="add",
    )(got, *state)


def tally_kernel(n, count, *refs):
    out = refs[-1]
    squares = jnp.zeros((8, 128), jnp.float32)
    for ref in refs[:count]:
        mean = ref[...] * (1.0 / n)
        squares = squares + jnp.sum((mean * mean).reshape(-1, 8, 128), axis=0)
    row = jnp.sum(squares, axis=0, keepdims=True)
    lane = 128 * lax.rem(lax.axis_index("mp"), 2)
    place = lax.broadcasted_iota(jnp.int32, (out.shape[0], 128), 0)
    out[...] = jnp.zeros_like(out)
    out[:, pl.ds(pl.multiple_of(lane, 128), 128)] = jnp.where(place == chunk_index(n, 0), row, 0.0)


def tally(values, state, n):
    columns = values[0].shape[1]
    return pl.pallas_call(
        functools.partial(tally_kernel, n, len(values)),
        out_shape=jax.ShapeDtypeStruct((-(-n // 8) * 8, columns), jnp.float32),
        in_specs=[VMEM] * (len(values) + len(state)),
        out_specs=VMEM,
        cost_estimate=estimate(sum(v.size for v in values), 40, 3),
        compiler_params=grant(0),
        name="tally",
    )(*values, *state)


def merge_kernel(how, count, *refs):
    table = refs[0][...]
    for ref in refs[1:count]:
        other = ref[ref.shape[0] - table.shape[0] :, :]
        table = table + other if how == "sum" else jnp.maximum(table, other)
    refs[-1][...] = table


def merge(tables, state, how):
    return pl.pallas_call(
        functools.partial(merge_kernel, how, len(tables)),
        out_shape=jax.ShapeDtypeStruct(tables[0].shape, jnp.float32),
        in_specs=[VMEM] * (len(tables) + len(state)),
        out_specs=VMEM,
        cost_estimate=estimate(tables[0].size, 12, 1),
        compiler_params=grant(0),
        name="merge",
    )(*tables, *state)


def load_kernel(piece_ref, table_ref, other_ref, *refs):
    out = refs[-1]
    rows = piece_ref.shape[0]
    out[:rows, :] = piece_ref[...]
    out[rows:, :] = jnp.maximum(table_ref[...], other_ref[...])


def load_rider(piece, table, other, state):
    shape = (piece.shape[0] + table.shape[0], piece.shape[1])
    return pl.pallas_call(
        load_kernel,
        out_shape=jax.ShapeDtypeStruct(shape, jnp.float32),
        in_specs=[VMEM] * (3 + len(state)),
        out_specs=VMEM,
        cost_estimate=estimate(piece.size, 12, 1),
        compiler_params=grant(0),
        name="load",
    )(piece, table, other, *state)


def unload_kernel(loaded_ref, *refs):
    refs[-1][...] = loaded_ref[: refs[-1].shape[0], :]


def unload_rider(loaded, rows, state):
    return pl.pallas_call(
        unload_kernel,
        out_shape=jax.ShapeDtypeStruct((rows, loaded.shape[1]), jnp.float32),
        in_specs=[VMEM] * (1 + len(state)),
        out_specs=VMEM,
        cost_estimate=estimate(loaded.size, 12, 1),
        compiler_params=grant(0),
        name="unload",
    )(loaded, *state)


def scale_kernel(max_norm, table_ref, *refs):
    norm = jnp.sqrt(jnp.sum(table_ref[...], keepdims=True))
    factor = jnp.minimum(1.0, max_norm / (norm + EPSILON))
    refs[-1][...] = jnp.broadcast_to(factor, refs[-1].shape)


def clip_factor(table, state, max_norm):
    return pl.pallas_call(
        functools.partial(scale_kernel, max_norm),
        out_shape=jax.ShapeDtypeStruct((8, table.shape[1]), jnp.float32),
        in_specs=[VMEM] * (1 + len(state)),
        out_specs=VMEM,
        cost_estimate=estimate(table.size, 12, 1),
        compiler_params=grant(0),
        name="scale",
    )(table, *state)


def update_kernel(n, pieces, n_outs, factor_ref, slow_ref, momentum_ref, *refs):
    count = len(pieces)
    sums = refs[:count]
    slow_out, momentum_out, fast_out = refs[count + n_outs : count + n_outs + 3]
    slow_buf, momentum_buf, fast_buf, sems = refs[count + n_outs + 3 :]
    factor = factor_ref[:1, :]
    copies = []
    at = 0
    for k, (back, start, rows) in enumerate(pieces):
        index = chunk_index(n, back)
        here, there = pl.ds(start, rows), pl.ds(at, rows)
        gradient = factor * (sums[k][:rows, :] * (1.0 / n))
        momentum_next = MOMENTUM_RATE * momentum_ref[index, here] + gradient
        slow_next = slow_ref[index, here] - OUTER_RATE * (gradient + MOMENTUM_RATE * momentum_next)
        slow_buf[there] = slow_next
        momentum_buf[there] = momentum_next
        fast_buf[there] = slow_next.astype(jnp.bfloat16)
        for j, (buf, out) in enumerate(
            ((slow_buf, slow_out), (momentum_buf, momentum_out), (fast_buf, fast_out))
        ):
            copy = pltpu.make_async_copy(buf.at[there], out.at[index, here], sems.at[j, k])
            copy.start(priority=j % 2)
            copies.append(copy)
        at += rows
    for copy in copies:
        copy.wait()


def update(factor, chunks, slow, momentum, outs, n):
    pieces = [(back, start, rows) for back, (start, rows), _ in chunks]
    count = len(chunks)
    columns = slow.shape[2]
    rows = sum(rows for _, _, rows in pieces)
    return pl.pallas_call(
        functools.partial(update_kernel, n, pieces, len(outs)),
        out_shape=(
            pltpu.HBM(slow.shape, jnp.float32),
            pltpu.HBM(slow.shape, jnp.float32),
            pltpu.HBM(slow.shape, jnp.bfloat16),
        ),
        in_specs=[VMEM, VMEM, VMEM] + [VMEM] * count + [HBM] * len(outs),
        out_specs=(HBM, HBM, HBM),
        scratch_shapes=[
            pltpu.VMEM((rows, columns), jnp.float32),
            pltpu.VMEM((rows, columns), jnp.float32),
            pltpu.VMEM((rows, columns), jnp.bfloat16),
            pltpu.SemaphoreType.DMA((3, count)),
        ],
        input_output_aliases={3 + count + k: k for k in range(len(outs))},
        cost_estimate=estimate(rows * columns, 22, 8),
        compiler_params=grant(rows * columns * 15),
        name="update",
    )(factor, slow, momentum, *[sums for _, _, sums in chunks], *outs)


def ring_order(n):
    if n % 2:
        return list(range(n))
    return [2 * k for k in range(n // 2)] + [n - 1 - 2 * k for k in range(n // 2)]


def ring_perm(n, m, back=False):
    order = ring_order(n)
    perm = []
    for k in range(n):
        for c in range(m):
            other = (k + 1) % n if (c % 2 == 0) != back else (k - 1) % n
            perm.append((order[k] * m + c, order[other] * m + c))
    return perm


def rides(n, m):
    return n % 2 == 0 and m > 1 and m & (m - 1) == 0


def exchanges(n, m):
    hops = STREAMS * (n - 1) - 1
    arrived = STREAMS * (1 + n // 2) + RIDER
    swap = [(c, c ^ 1) for c in range(m)]
    steps = [(swap, STREAMS, STREAMS + RIDER), (swap, arrived + 1, arrived + 3)]
    bit = 2
    while bit < m:
        start = steps[-1][2]
        steps.append(([(c, c ^ bit) for c in range(m)], start, min(start + STREAMS - 1, hops)))
        bit *= 2
    return steps


def back_slot(n, m):
    return exchanges(n, m)[-1][1] if rides(n, m) else STREAMS * (n - 1) - 2


def body(slow_weights, fast_weights, momentum):
    n, m = lax.axis_size("dp"), lax.axis_size("mp")
    rows, columns = slow_weights.shape[1:]
    max_norm = CLIP_LEVEL * math.sqrt(slow_weights.size * m)
    depth = rows // n
    slow = slow_weights.reshape(n, depth, columns)
    fast = fast_weights.reshape(n, depth, columns)
    moment = momentum.reshape(n, depth, columns)
    parts = split(depth)
    perm, back_perm = ring_perm(n, m), ring_perm(n, m, back=True)
    riding = rides(n, m)
    steps = exchanges(n, m) if riding else []

    def hop(value, pairs=perm):
        return lax.ppermute(value, ("dp", "mp"), pairs)

    held = list(first_pieces(slow, fast, n, parts[:FIRST]))
    held += [own_piece(slow, fast, n, part) for part in parts[FIRST:]]
    for step in range(n - 1):
        state = (slow, fast) if step < LATE else (slow, fast, moment)
        for s, part in enumerate(parts):
            held[s] = add_piece(hop(held[s]), state, n, step + 2, part)

    state = (slow, moment)
    chunks = [[(0, part, held[s]) for s, part in enumerate(parts)]]
    table = tally([sums for _, _, sums in chunks[0]], state, n)
    if not riding:
        table = lax.psum(table, ("dp", "mp"))
    got = [None] * len(steps)

    def swap(j, value):
        return lax.ppermute(value, "mp", steps[j][0])

    hops = STREAMS * (n - 1) - 1
    for slot in range(hops + 1):
        step, s = divmod(slot, STREAMS)
        if slot == back_slot(n, m):
            final = hop(chunks[0][-1][2], back_perm)
        for j, (_, start, end) in enumerate(steps):
            if slot == end and j == 0:
                held[s] = load_rider(held[s], table, got[j], state)
            elif slot == end:
                table = merge([table, got[j]], state, "max" if j == 1 else "sum")
            if slot == start:
                if j == 1:
                    riders = [chunk[RIDER][2] for chunk in chunks[2 : 2 + n // 2]]
                    table = merge([table, got[0]] + riders, state, "max")
                got[j] = swap(j, table)
        if slot == hops:
            break
        if riding and s == RIDER and step == 1 + n // 2:
            held[s] = unload_rider(held[s], parts[s][1], state)
        held[s] = hop(held[s])
        if s == 0:
            chunks.append([])
        chunks[-1].append((step + 1, parts[s], held[s]))

    chunks[0].append((n - 1, parts[-1], final))
    factor = clip_factor(table, state, max_norm)
    mine = [piece for chunk in chunks[:-1] for piece in chunk]
    outs = update(factor, mine, slow, moment, (), n)
    outs = update(factor, chunks[-1], slow, moment, outs, n)
    slow_next, momentum_next, fast_next = outs
    return (
        slow_next.reshape(slow_weights.shape),
        momentum_next.reshape(momentum.shape),
        fast_next.reshape(fast_weights.shape),
    )


def solution(mesh):
    in_specs = (P(None, None, "mp"), P("dp", None, None, "mp"), P(None, None, "mp"))
    out_specs = (P(None, None, "mp"), P(None, None, "mp"), P("dp", None, None, "mp"))
    return jax.shard_map(body, mesh=mesh, in_specs=in_specs, out_specs=out_specs, check_vma=False)
```
